256 devices in a mesh: tm: 4 (over y), blk: 64 (over x, z, core).
Axes of the slice: x: 4, y: 4, z: 8, core: 2. Of those that a mesh axis runs over, the one named last changes fastest.
Arguments:
- chi_bar: bfloat16 [4, 64, 24, 128, 128], P('tm', 'blk'), may hold values from -0.023925781 to 0.023925781
- cos_table: int32 [8, 4], replicated, may hold values from -1024 to 1024
- partner: int32 [64, 24], P('blk'), may hold values from 0 to 63, all different within a row
- tensor: bfloat16 [8192, 2, 2048], P('blk'), may hold values from -6 to 6
- dens_tensor: bfloat16 [8192, 2, 2048], P('blk'), may hold values from -6 to 6
- decay: float32 [8, 2, 2048], P('tm'), may hold values from 0.1 to 1
Outputs:
- tensor_grad: bfloat16 [8, 8192, 2, 2048], P('tm', 'blk')
- density_grad: float32 [8192, 128], P('blk')
The draws below stay inside these ranges and needn't reach their ends.
Inputs may be any that keep to these rules, and one draw needn't show every extreme that they name: `partner`: each row names 24 different blocks; every block is named by some row.
All inputs are finite; a program needn't handle non-finite values.
Results may differ from the reference program's by a relative error of at most 0.011.
Values may be sent and summed in bfloat16 or wider, within the bound.
No kernel may reach another device: no remote copies, remote signals or barrier semaphores. Data moves between devices by JAX's collectives and lax.ppermute only.
A program may use at most 64 MiB of HBM per device.

```python
import math
import jax
import jax.numpy as jnp
from jax import lax

BLOCK = 128
TILE_COLS = 2048
TILES = 2
NFREQ = 4
NTIME = 8
NPAIR = 24
AUX = 8192
N_BLK = 64


def with_ends(drawn, key, least, largest):
    longest = drawn.shape.index(max(drawn.shape))
    spots = []
    for shift in (0, 1):
        where = [jax.random.randint(jax.random.fold_in(key, axis), (), 0, length) for axis, length in enumerate(drawn.shape)]
        where[longest] = (where[longest] + shift) % drawn.shape[longest]
        spots.append(tuple(where))
    return drawn.at[spots[0]].set(least).at[spots[1]].set(largest)


def steps_of(own_key, extent, cuts, low, high):
    factor_of, own = 1.0, jax.random.fold_in(own_key, 6)
    for dim, shards_of in cuts:
        steps = jnp.exp(jax.random.uniform(jax.random.fold_in(own, dim), (shards_of,), jnp.float32, low / len(cuts), high / len(cuts)))
        factor_of = factor_of * jnp.repeat(steps, extent[dim] // shards_of).reshape([-1 if axis == dim else 1 for axis in range(len(extent))])
    return factor_of


def distinct(stream_key, rows, count, top, lift):
    sequence = jax.random.permutation(jax.random.fold_in(stream_key, 1), count)
    pull = sequence
    for power in range(3):
        pull = pull * pull // count
    pull = pull * lift // count
    tickets = jax.random.randint(jax.random.fold_in(stream_key, 2), (rows, count), 0, 4096) + pull
    sure = jax.random.permutation(jax.random.fold_in(stream_key, 3), rows)[jnp.arange(count) % rows]
    tickets = jnp.where(jnp.arange(rows)[:, None] == sure[None, :], 1 << 14, tickets)
    merit = tickets * count + jnp.arange(count)
    return lax.top_k(merit.astype(jnp.int32), top)[1].astype(jnp.int32)


def gaussian(own_key, extent, scale, most, pieces=(), held_as=jnp.bfloat16):
    array = scale * jax.random.normal(own_key, extent, jnp.float32)
    if pieces:
        array = array * steps_of(own_key, extent, pieces, -0.22, 0.18)
    return jnp.clip(array, -most, most).astype(held_as)


def setup_inputs(seed: int = 0) -> dict:
    seeds = jax.random.split(jax.random.key(seed), 7)
    chi_bar = gaussian(seeds[0], (NFREQ, N_BLK, NPAIR, BLOCK, BLOCK), 0.004, 0.023925781, ((0, 4), (1, 64)))
    cos_table = with_ends(jax.random.randint(seeds[1], (NTIME, NFREQ), -1024, 1025), jax.random.fold_in(seeds[1], 1), -1024, 1024).astype(jnp.int32)
    partner = distinct(seeds[2], N_BLK, N_BLK, NPAIR, 6144)
    tensor = gaussian(seeds[3], (AUX, TILES, TILE_COLS), 1.0, 6.0, ((0, 64),))
    dens_tensor = gaussian(seeds[4], (AUX, TILES, TILE_COLS), 1.0, 6.0, ((0, 64),))
    decay = jnp.clip(jnp.exp(math.log(1.0) - 2.3025851 * jax.random.uniform(seeds[5], (NTIME, TILES, TILE_COLS), jnp.float32) ** steps_of(seeds[5], (NTIME, TILES, TILE_COLS), ((0, 4),), -0.2, 0.2)), 0.1, 1.0)
    return {"chi_bar": chi_bar, "cos_table": cos_table, "partner": partner, "tensor": tensor, "dens_tensor": dens_tensor, "decay": decay}


def reference(chi_bar, cos_table, partner, tensor, dens_tensor, decay):
    hp = lax.Precision.HIGHEST
    weights = cos_table.astype(jnp.float32) / 1024.0
    width = TILES * TILE_COLS
    inv_width = 1.0 / math.sqrt(width)
    chi_full = chi_bar.astype(jnp.float32)
    onehot = (partner[:, :, None] == jnp.arange(N_BLK, dtype=jnp.int32)[None, None, :]).astype(jnp.float32)
    tens = tensor.reshape(N_BLK, BLOCK, width)
    dens = dens_tensor.reshape(N_BLK, BLOCK, width)
    tens_f = tens.astype(jnp.float32)

    def one_time(index):
        gbar = jnp.einsum('w,wqkab->qkab', weights[index], chi_full, precision=hp).astype(jnp.bfloat16)
        factor = decay[index].reshape(1, 1, width)
        scaled = (tens_f * factor).astype(jnp.bfloat16).astype(jnp.float32)
        dscaled = (dens.astype(jnp.float32) * factor).astype(jnp.bfloat16).astype(jnp.float32)
        metric = (jnp.einsum('qaj,qbj->qab', tens_f, dscaled) * inv_width).astype(jnp.bfloat16)
        term = jnp.einsum('qkab,qbc->qkac', gbar.astype(jnp.float32), metric.astype(jnp.float32))
        collected = jnp.einsum('qkp,qkac->pac', onehot, term, precision=hp).astype(jnp.bfloat16).astype(jnp.float32)
        grad = jnp.einsum('pab,pbj->paj', collected, scaled) + jnp.einsum('pba,pbj->paj', collected, dscaled)
        grad = grad.astype(jnp.bfloat16)
        dpart = jnp.einsum('paj,pbj->pab', grad.astype(jnp.float32), dscaled) * inv_width
        return (grad, dpart)
    grads, dparts = lax.map(one_time, jnp.arange(NTIME, dtype=jnp.int32))
    tensor_grad = grads.reshape(NTIME, AUX, TILES, TILE_COLS)
    density_grad = lax.optimization_barrier(jnp.sum(dparts, axis=0)).reshape(AUX, BLOCK)
    return (tensor_grad, density_grad)
```

```python
import math

import jax
import jax.numpy as jnp
from jax import lax
from jax.experimental import pallas as pl
from jax.experimental.pallas import tpu as pltpu
from jax.sharding import PartitionSpec as P

CHUNKS = 2
NX, NZ, NC, NY = 4, 8, 2, 4

bf16 = jnp.bfloat16
f32 = jnp.float32
VMEM = pltpu.VMEM
SMEM = pltpu.SMEM


def blk_of(x, z, c):
    return (x * NZ + z) * NC + c


CHIPS = [(x, z) for x in range(NX) for z in range(NZ)]
CORE_SWAP = [(blk_of(x, z, c), blk_of(x, z, 1 - c)) for x, z in CHIPS for c in range(NC)]
X_GROUPS = [[blk_of(x, z, c) for x in range(NX)] for z in range(NZ) for c in range(NC)]
Z_GROUPS = [[blk_of(x, z, c) for z in range(NZ)] for x in range(NX) for c in range(NC)]


def y_shift(d):
    return [(i, (i + d) % NY) for i in range(NY)]


def call(body, out_shape, *args, smem=(), flops=0, name=None):
    in_specs = [pl.BlockSpec(memory_space=SMEM if i in smem else VMEM) for i in range(len(args))]
    outs = out_shape if isinstance(out_shape, (list, tuple)) else [out_shape]
    out_specs = [pl.BlockSpec(memory_space=VMEM) for _ in outs]
    size = sum(math.prod(a.shape) * a.dtype.itemsize for a in args)
    return pl.pallas_call(
        body,
        out_shape=out_shape,
        in_specs=in_specs,
        out_specs=out_specs if isinstance(out_shape, (list, tuple)) else out_specs[0],
        cost_estimate=pl.CostEstimate(flops=flops, bytes_accessed=size, transcendentals=0),
        name=name,
    )(*args)


def prep_body(tens_ref, dens_ref, decay_ref, scaled_ref, dscaled_ref, metric_ref, gram_ref):
    width = tens_ref.shape[1]
    nt = (((1,), (1,)), ((), ()))
    inv_width = 1.0 / math.sqrt(width)
    tens = tens_ref[...]
    for t in range(decay_ref.shape[0]):
        factor = decay_ref[pl.ds(t, 1), :]
        s = (tens.astype(f32) * factor).astype(bf16)
        d = (dens_ref[...].astype(f32) * factor).astype(bf16)
        scaled_ref[t] = s
        dscaled_ref[t] = d
        m = lax.dot_general(tens, d, nt, preferred_element_type=f32)
        metric_ref[t] = (m * inv_width).astype(bf16)
        for i, left in enumerate((s, d)):
            g = lax.dot_general(left, d, nt, preferred_element_type=f32) * inv_width
            hi = g.astype(bf16)
            gram_ref[t, i, :, 0:128] = hi
            gram_ref[t, i, :, 128:256] = (g - hi.astype(f32)).astype(bf16)


def term_body(part_ref, wts_ref, c0_ref, c1_ref, c2_ref, c3a_ref, c3b_ref, metric_ref, send_ref, keep_ref):
    pairs, rows = c0_ref.shape[0], c0_ref.shape[1]
    group = 6
    my_core = part_ref[pairs]
    zero = jnp.zeros((rows, 128), bf16)

    def clear(s, _):
        for t in range(2):
            send_ref[s, t] = zero
            keep_ref[s, t] = zero
        return 0

    lax.fori_loop(0, send_ref.shape[0], clear, 0)
    for g in range(pairs // group):
        k0 = g * group
        ks = slice(k0, k0 + group)
        last = c3a_ref[ks] if g < pairs // group // 2 else c3b_ref[slice(k0 - pairs // 2, k0 - pairs // 2 + group)]
        chis = [r.astype(f32) for r in (c0_ref[ks], c1_ref[ks], c2_ref[ks], last)]
        for t in range(2):
            mixed = chis[0] * wts_ref[t, 0]
            for i in range(1, 4):
                mixed = mixed + chis[i] * wts_ref[t, i]
            mixed = mixed.astype(bf16).reshape(group * rows, 128)
            prod = jnp.dot(mixed, metric_ref[t], preferred_element_type=f32).astype(bf16)
            for j in range(group):
                p = part_ref[k0 + j]
                piece = prod[j * rows : (j + 1) * rows]

                @pl.when((p & 1) == my_core)
                def _():
                    keep_ref[p >> 1, t] = piece

                @pl.when((p & 1) != my_core)
                def _():
                    send_ref[p >> 1, t] = piece


def final_body(scaled_ref, dscaled_ref, col, grad_ref):
    tn = (((0,), (0,)), ((), ()))
    step = 512
    for t in range(2):
        c = col[t]
        for j in range(scaled_ref.shape[2] // step):
            cols = slice(j * step, (j + 1) * step)
            g = jnp.dot(c, scaled_ref[t, :, cols], preferred_element_type=f32)
            g = g + lax.dot_general(c, dscaled_ref[t, :, cols], tn, preferred_element_type=f32)
            grad_ref[t, :, cols] = g.astype(bf16)


def density_body(col_ref, gram_ref, out_ref):
    tn = (((0,), (0,)), ((), ()))
    total = jnp.zeros((128, 256), f32)
    for t in range(2):
        c = col_ref[t]
        total = total + jnp.dot(c, gram_ref[t, 0], preferred_element_type=f32)
        total = total + lax.dot_general(c, gram_ref[t, 1], tn, preferred_element_type=f32)
    out_ref[...] = (total[:, 0:128] + total[:, 128:256]).astype(bf16)


def sds(shape, dtype=bf16):
    return jax.ShapeDtypeStruct(shape, dtype)


def on_device(chi_bar, cos_table, partner, tensor, dens_tensor, decay):
    pairs = chi_bar.shape[2]
    half = pairs // 2
    times = decay.shape[0]
    block = tensor.shape[0]
    width = tensor.shape[1] * tensor.shape[2]
    me_y = lax.axis_index("tm")
    core = lax.axis_index("blk") % NC

    table = lax.dynamic_slice_in_dim(cos_table, me_y * times, times, 0).astype(f32) / 1024.0
    order = jnp.stack([me_y, (me_y + 3) % NY, (me_y + 1) % NY, (me_y + 2) % NY])
    wts = jnp.take(table, order, axis=1)
    part = jnp.concatenate([partner[0], core[None].astype(jnp.int32)])

    rows = block // CHUNKS
    up, down = y_shift(1), y_shift(-1)
    mine = [chi_bar[0, 0, :, c * rows : (c + 1) * rows, :] for c in range(CHUNKS)]
    from_low = [lax.ppermute(m, "tm", up) for m in mine]
    from_high = [lax.ppermute(m, "tm", down) for m in mine]
    far_a = [lax.ppermute(m[:half], "tm", up) for m in from_low]
    far_b = [lax.ppermute(m[half:], "tm", down) for m in from_high]

    scaled, dscaled, metric, gram = call(
        prep_body,
        [
            sds((times, block, width)),
            sds((times, block, width)),
            sds((times, block, block)),
            sds((times, 2, block, 2 * block)),
        ],
        tensor.reshape(block, width),
        dens_tensor.reshape(block, width),
        decay.reshape(times, width),
        flops=10**9,
        name="prep",
    )
    collected = []
    for c in range(CHUNKS):
        shape = (NX * NZ, times, rows, block)
        send, keep = call(
            term_body,
            [sds(shape), sds(shape)],
            part,
            wts,
            mine[c],
            from_low[c],
            from_high[c],
            far_a[c],
            far_b[c],
            metric,
            smem=(0, 1),
            flops=10**9,
            name="term",
        )
        both = (keep.astype(f32) + lax.ppermute(send, "blk", CORE_SWAP).astype(f32)).astype(bf16)
        both = both.reshape(NX, NZ, times, rows, block)
        both = lax.all_to_all(both, "blk", 0, 0, axis_index_groups=X_GROUPS, tiled=True)
        both = both.astype(f32).sum(axis=0).astype(bf16)
        both = lax.all_to_all(both, "blk", 0, 0, axis_index_groups=Z_GROUPS, tiled=True)
        collected.append(both.astype(f32).sum(axis=0).astype(bf16))
    col = jnp.concatenate(collected, axis=1)
    dpart = call(density_body, sds((block, block)), col, gram, flops=10**8, name="density")
    density = dpart.astype(f32)
    for d in range(1, NY):
        density = density + lax.ppermute(dpart, "tm", y_shift(d)).astype(f32)
    grad = call(final_body, sds((times, block, width)), scaled, dscaled, col, flops=10**9, name="final")
    return (grad.reshape(times, block, tensor.shape[1], tensor.shape[2]), density)


def solution(mesh):
    return jax.shard_map(
        on_device,
        mesh=mesh,
        in_specs=(
            P("tm", "blk", None, None, None),
            P(),
            P("blk", None),
            P("blk", None, None),
            P("blk", None, None),
            P("tm", None, None),
        ),
        out_specs=(P("tm", "blk", None, None), P("blk", None)),
        check_vma=False,
    )
```

```python
import math

import jax
import jax.numpy as jnp
from jax import lax
from jax.experimental import pallas as pl
from jax.experimental.pallas import tpu as pltpu
from jax.sharding import PartitionSpec as P


CHUNKS = (64, 64)
LAST_BY_GROUP = True
NX, NZ, NC, NY = 4, 8, 2, 4

bf16 = jnp.bfloat16
f32 = jnp.float32
VMEM = pltpu.VMEM
SMEM = pltpu.SMEM


def blk_of(x, z, c):
    return (x * NZ + z) * NC + c


CHIPS = [(x, z) for x in range(NX) for z in range(NZ)]
CORE_SWAP = [(blk_of(x, z, c), blk_of(x, z, 1 - c)) for x, z in CHIPS for c in range(NC)]
Z_GROUPS = [[blk_of(x, z, c) for z in range(NZ)] for x in range(NX) for c in range(NC)]


def x_shift(d):
    return [(blk_of(x, z, c), blk_of((x + d) % NX, z, c)) for x, z in CHIPS for c in range(NC)]


def z_shift(d):
    return [(blk_of(x, z, c), blk_of(x, (z + d) % NZ, c)) for x, z in CHIPS for c in range(NC)]


def y_shift(d):
    return [(i, (i + d) % NY) for i in range(NY)]


def call(body, out_shape, *args, smem=(), flops=0, mib=16):
    many = isinstance(out_shape, (list, tuple))
    size = sum(math.prod(a.shape) * a.dtype.itemsize for a in args)
    out_spec = pl.BlockSpec(memory_space=VMEM)
    return pl.pallas_call(
        body,
        out_shape=out_shape,
        in_specs=[pl.BlockSpec(memory_space=SMEM if i in smem else VMEM) for i in range(len(args))],
        out_specs=[out_spec] * len(out_shape) if many else out_spec,
        cost_estimate=pl.CostEstimate(flops=flops, bytes_accessed=size, transcendentals=0),
        compiler_params=pltpu.CompilerParams(vmem_limit_bytes=mib << 20),
    )(*args)


def prep_body(tens_ref, dens_ref, decay_ref, metric_ref, gram_ref):
    nt = (((1,), (1,)), ((), ()))
    inv_width = 1.0 / math.sqrt(tens_ref.shape[1])
    tens = tens_ref[...]
    for t in range(decay_ref.shape[0]):
        factor = decay_ref[pl.ds(t, 1), :]
        s = (tens.astype(f32) * factor).astype(bf16)
        d = (dens_ref[...].astype(f32) * factor).astype(bf16)
        m = lax.dot_general(tens, d, nt, preferred_element_type=f32)
        metric_ref[t] = (m * inv_width).astype(bf16)
        for i, left in enumerate((s, d)):
            g = lax.dot_general(left, d, nt, preferred_element_type=f32) * inv_width
            hi = g.astype(bf16)
            gram_ref[t, i, :, 0:128] = hi
            gram_ref[t, i, :, 128:256] = (g - hi.astype(f32)).astype(bf16)


def term_body(part_ref, cos_ref, metric_ref, *refs):
    chi_refs, (send_ref, keep_ref) = (refs[0:4], refs[4:8]), refs[8:]
    half, rows = refs[0].shape[0], refs[0].shape[1]
    group = 6
    me_y = lax.axis_index("tm")
    my_core = lax.axis_index("blk") & 1
    spare = keep_ref.shape[0] - 1
    zero = jnp.zeros((rows, 128), bf16)
    weights = [
        [cos_ref[me_y * 2 + t, (me_y + d) & 3].astype(f32) * (1.0 / 1024.0) for d in (0, 3, 1, 2)]
        for t in range(2)
    ]

    def clear(s, _):
        for t in range(2):
            send_ref[s, t] = zero
            keep_ref[s, t] = zero
        return 0

    lax.fori_loop(0, send_ref.shape[0], clear, 0)
    for k0 in range(0, 2 * half, group):
        ks = slice(k0 % half, k0 % half + group)
        chis = [r[ks].astype(f32) for r in chi_refs[k0 // half]]
        for t in range(2):
            mixed = chis[0] * weights[t][0]
            for i in range(1, 4):
                mixed = mixed + chis[i] * weights[t][i]
            mixed = mixed.astype(bf16).reshape(group * rows, 128)
            prod = jnp.dot(mixed, metric_ref[t], preferred_element_type=f32).astype(bf16)
            for j in range(group):
                p = part_ref[0, k0 + j]
                piece = prod[j * rows : (j + 1) * rows]
                own = (p & 1) == my_core
                keep_ref[jnp.where(own, p >> 1, spare), t] = piece
                send_ref[jnp.where(own, spare, p >> 1), t] = piece


def add_rows(a_ref, b_ref, i):
    return (a_ref[i].astype(f32) + b_ref[i].astype(f32)).astype(bf16)


def add_split_body(a_ref, b_ref, *out_refs):
    my_x = lax.axis_index("blk") >> 4
    for d, out_ref in enumerate(out_refs):
        first = ((my_x + d) & 3) * NZ

        def body(i, _):
            out_ref[i] = add_rows(a_ref, b_ref, first + i)
            return 0

        lax.fori_loop(0, NZ, body, 0, unroll=4)


def sum_split_body(a_ref, b_ref, c_ref, d_ref, *out_refs):
    my_z = (lax.axis_index("blk") >> 1) & 7
    for d, out_ref in enumerate(out_refs):
        i = (my_z + d) & 7
        low = a_ref[i].astype(f32) + b_ref[i].astype(f32)
        out_ref[...] = (low + (c_ref[i].astype(f32) + d_ref[i].astype(f32))).astype(bf16)


def sum_body(a_ref, b_ref, c_ref, d_ref, out_ref):
    def body(i, _):
        low = a_ref[i].astype(f32) + b_ref[i].astype(f32)
        out_ref[i] = (low + (c_ref[i].astype(f32) + d_ref[i].astype(f32))).astype(bf16)
        return 0

    lax.fori_loop(0, NZ, body, 0, unroll=4)


def sum_all_body(*refs):
    total = refs[0][...].astype(f32)
    for r in refs[1:-1]:
        total = total + r[...].astype(f32)
    refs[-1][...] = total.astype(bf16)


def sum_lead_body(in_ref, out_ref):
    step = 16
    for t in range(out_ref.shape[0]):
        for r in range(0, out_ref.shape[1], step):
            rows = slice(r, r + step)
            total = in_ref[0, t, rows].astype(f32)
            for i in range(1, in_ref.shape[0]):
                total = total + in_ref[i, t, rows].astype(f32)
            out_ref[t, rows] = total.astype(bf16)


def spread(c, side):
    shape = (2 * c.shape[0], c.shape[0])
    r = lax.broadcasted_iota(jnp.int32, shape, 0)
    a = lax.broadcasted_iota(jnp.int32, shape, 1)
    pick = jnp.where((r >> 1) == a, 1.0, 0.0).astype(bf16)
    c = lax.dot_general(pick, c, (((1,), (side,)), ((), ())), preferred_element_type=f32)
    even = (r & 1) == 0
    return jnp.concatenate([jnp.where(even, c, 0.0), jnp.where(even, 0.0, c)], axis=1).astype(bf16)


def gather_rows(col_refs, t):
    return jnp.concatenate([r[t] for r in col_refs], axis=0)


def final_body(tens0_ref, tens1_ref, dens0_ref, dens1_ref, decay0_ref, decay1_ref, *refs):
    col_refs, grad_ref, mix_ref = refs[:-2], refs[-2], refs[-1]
    times = grad_ref.shape[0]

    @pl.when(pl.program_id(0) == 0)
    def _():
        for t in range(times):
            c = gather_rows(col_refs, t)
            for side in range(2):
                mix_ref[t, side] = spread(c, side)

    def scaled(refs, t):
        return jnp.concatenate(
            [(r[...].astype(f32) * f[pl.ds(t, 1), :]).astype(bf16) for r, f in zip(refs, (decay0_ref, decay1_ref))], axis=0
        )

    for t in range(times):
        g = jnp.dot(mix_ref[t, 0], scaled((tens0_ref, tens1_ref), t), preferred_element_type=f32)
        g = g + jnp.dot(mix_ref[t, 1], scaled((dens0_ref, dens1_ref), t), preferred_element_type=f32)
        grad_ref[t] = g.astype(bf16).reshape(g.shape[0] // 2, 2, g.shape[1])


def final(tens, dens, decay, collected):
    block, width = tens.shape
    times = decay.shape[0]
    half, step = width // 2, 512
    steps = half // step
    views = [pl.BlockSpec((block, step), lambda i, j=j: (0, i + j * steps)) for j in range(2)]
    decays = [pl.BlockSpec((times, step), lambda i, j=j: (0, i + j * steps)) for j in range(2)]
    whole = [pl.BlockSpec(c.shape, lambda i: (0, 0, 0)) for c in collected]
    return pl.pallas_call(
        final_body,
        grid=(steps,),
        out_shape=sds((times, block, 2, half)),
        in_specs=views * 2 + decays + whole,
        out_specs=pl.BlockSpec((times, block, 2, step), lambda i: (0, 0, 0, i)),
        scratch_shapes=[VMEM((times, 2, 2 * block, 2 * block), bf16)],
        cost_estimate=pl.CostEstimate(flops=10**9, bytes_accessed=4 << 20, transcendentals=0),
        compiler_params=pltpu.CompilerParams(vmem_limit_bytes=16 << 20),
        name="final",
    )(tens, tens, dens, dens, decay, decay, *collected)


def density_body(gram_ref, *refs):
    col_refs, out_ref = refs[:-1], refs[-1]
    tn = (((0,), (0,)), ((), ()))
    total = jnp.zeros((128, 256), f32)
    for t in range(2):
        c = gather_rows(col_refs, t)
        total = total + jnp.dot(c, gram_ref[t, 0], preferred_element_type=f32)
        total = total + lax.dot_general(c, gram_ref[t, 1], tn, preferred_element_type=f32)
    out_ref[...] = (total[:, 0:128] + total[:, 128:256]).astype(bf16)


def density_sum_body(a_ref, b_ref, c_ref, d_ref, out_ref):
    out_ref[...] = (a_ref[...].astype(f32) + b_ref[...].astype(f32)) + (c_ref[...].astype(f32) + d_ref[...].astype(f32))


def sds(shape, dtype=bf16):
    return jax.ShapeDtypeStruct(shape, dtype)


def exchange(value, groups):
    return lax.all_to_all(value, "blk", 0, 0, axis_index_groups=groups, tiled=True)


def work(chi_bar, cos_table, partner, tensor, dens_tensor, decay):
    pairs = chi_bar.shape[2]
    half = pairs // 2
    times = decay.shape[0]
    block = tensor.shape[0]
    width = tensor.shape[1] * tensor.shape[2]
    up, down = y_shift(1), y_shift(-1)

    chis = []
    start = 0
    for rows in CHUNKS:
        mine = [chi_bar[0, 0, h : h + half, start : start + rows, :] for h in (0, half)]
        low_a = lax.ppermute(mine[0], "tm", up)
        high_b = lax.ppermute(mine[1], "tm", down)
        low_b = lax.ppermute(mine[1], "tm", up)
        high_a = lax.ppermute(mine[0], "tm", down)
        far_a = lax.ppermute(low_a, "tm", up)
        far_b = lax.ppermute(high_b, "tm", down)
        chis.append((mine[0], low_a, high_a, far_a, mine[1], low_b, high_b, far_b))
        start += rows

    inputs = (tensor.reshape(block, width), dens_tensor.reshape(block, width), decay.reshape(times, width))
    metric, gram = call(
        prep_body, [sds((times, block, block)), sds((times, 2, block, 2 * block))], *inputs, flops=10**9
    )
    collected = []
    for c, rows in enumerate(CHUNKS):
        shape = sds((NX * NZ + 1, times, rows, block))
        piece = sds((NZ, times, rows, block))
        small = sds((times, rows, block))
        send, keep = call(term_body, [shape, shape], partner, cos_table, metric, *chis[c], smem=(0, 1), flops=10**9)
        other = lax.ppermute(send, "blk", CORE_SWAP)
        both = call(add_split_body, [piece] * NX, keep, other, flops=10**7)
        moved = [lax.ppermute(both[d], "blk", x_shift(d)) for d in range(1, NX)]
        if c == 0 or not LAST_BY_GROUP:
            both = call(sum_split_body, [small] * NZ, both[0], *moved, flops=10**7)
            moved = [lax.ppermute(both[d], "blk", z_shift(d)) for d in range(1, NZ)]
            collected.append(call(sum_all_body, small, both[0], *moved, flops=10**7))
        else:
            both = call(sum_body, piece, both[0], *moved, flops=10**7)
            both = exchange(both, Z_GROUPS)
            collected.append(call(sum_lead_body, small, both, flops=10**7))
    dpart = call(density_body, sds((block, block)), gram, *collected, flops=10**8)
    parts = [lax.ppermute(dpart, "tm", y_shift(d)) for d in range(1, NY)]
    grad = final(*inputs, collected)
    density = call(density_sum_body, sds((block, block), f32), dpart, *parts)
    return (grad, density)


def solution(mesh):
    return jax.shard_map(
        work,
        mesh=mesh,
        in_specs=(
            P("tm", "blk", None, None, None),
            P(),
            P("blk", None),
            P("blk", None, None),
            P("blk", None, None),
            P("tm", None, None),
        ),
        out_specs=(P("tm", "blk", None, None), P("blk", None)),
        check_vma=False,
    )
```

```python
import math

import jax
import jax.numpy as jnp
from jax import lax
from jax.experimental import pallas as pl
from jax.experimental.pallas import tpu as pltpu
from jax.sharding import PartitionSpec as P


CHUNKS = (64, 64)
NX, NZ, NC, NY = 4, 8, 2, 4

bf16 = jnp.bfloat16
f32 = jnp.float32
VMEM = pltpu.VMEM
SMEM = pltpu.SMEM


def blk_of(x, z, c):
    return (x * NZ + z) * NC + c


CHIPS = [(x, z) for x in range(NX) for z in range(NZ)]
CORE_SWAP = [(blk_of(x, z, c), blk_of(x, z, 1 - c)) for x, z in CHIPS for c in range(NC)]
Z_GROUPS = [[blk_of(x, z, c) for z in range(NZ)] for x in range(NX) for c in range(NC)]


def x_shift(d):
    return [(blk_of(x, z, c), blk_of((x + d) % NX, z, c)) for x, z in CHIPS for c in range(NC)]


def y_shift(d):
    return [(i, (i + d) % NY) for i in range(NY)]


def call(body, out_shape, *args, smem=(), flops=0, mib=16):
    many = isinstance(out_shape, (list, tuple))
    size = sum(math.prod(a.shape) * a.dtype.itemsize for a in args)
    out_spec = pl.BlockSpec(memory_space=VMEM)
    return pl.pallas_call(
        body,
        out_shape=out_shape,
        in_specs=[pl.BlockSpec(memory_space=SMEM if i in smem else VMEM) for i in range(len(args))],
        out_specs=[out_spec] * len(out_shape) if many else out_spec,
        cost_estimate=pl.CostEstimate(flops=flops, bytes_accessed=size, transcendentals=0),
        compiler_params=pltpu.CompilerParams(vmem_limit_bytes=mib << 20),
    )(*args)


def prep_body(tens_ref, dens_ref, decay_ref, metric_ref, gram_ref):
    nt = (((1,), (1,)), ((), ()))
    inv_width = 1.0 / math.sqrt(tens_ref.shape[1])
    tens = tens_ref[...]
    for t in range(decay_ref.shape[0]):
        factor = decay_ref[pl.ds(t, 1), :]
        s = (tens.astype(f32) * factor).astype(bf16)
        d = (dens_ref[...].astype(f32) * factor).astype(bf16)
        m = lax.dot_general(tens, d, nt, preferred_element_type=f32)
        metric_ref[t] = (m * inv_width).astype(bf16)
        for i, left in enumerate((s, d)):
            g = lax.dot_general(left, d, nt, preferred_element_type=f32) * inv_width
            hi = g.astype(bf16)
            gram_ref[t, i, :, 0:128] = hi
            gram_ref[t, i, :, 128:256] = (g - hi.astype(f32)).astype(bf16)


def term_body(part_ref, cos_ref, metric_ref, *refs):
    chi_refs, (send_ref, keep_ref) = (refs[0:4], refs[4:8]), refs[8:]
    half, rows = refs[0].shape[0], refs[0].shape[1]
    group = 6
    me_y = lax.axis_index("tm")
    my_core = lax.axis_index("blk") & 1
    spare = keep_ref.shape[0] - 1
    zero = jnp.zeros((rows, 128), bf16)
    weights = [
        [cos_ref[me_y * 2 + t, (me_y + d) & 3].astype(f32) * (1.0 / 1024.0) for d in (0, 3, 1, 2)]
        for t in range(2)
    ]

    def clear(s, _):
        for t in range(2):
            send_ref[s, t] = zero
            keep_ref[s, t] = zero
        return 0

    lax.fori_loop(0, send_ref.shape[0], clear, 0)
    for k0 in range(0, 2 * half, group):
        ks = slice(k0 % half, k0 % half + group)
        chis = [r[ks].astype(f32) for r in chi_refs[k0 // half]]
        for t in range(2):
            mixed = chis[0] * weights[t][0]
            for i in range(1, 4):
                mixed = mixed + chis[i] * weights[t][i]
            mixed = mixed.astype(bf16).reshape(group * rows, 128)
            prod = jnp.dot(mixed, metric_ref[t], preferred_element_type=f32).astype(bf16)
            for j in range(group):
                p = part_ref[0, k0 + j]
                piece = prod[j * rows : (j + 1) * rows]
                own = (p & 1) == my_core
                keep_ref[jnp.where(own, p >> 1, spare), t] = piece
                send_ref[jnp.where(own, spare, p >> 1), t] = piece


def add_rows(a_ref, b_ref, i):
    return (a_ref[i].astype(f32) + b_ref[i].astype(f32)).astype(bf16)


def add_split_body(a_ref, b_ref, *out_refs):
    my_x = lax.axis_index("blk") >> 4
    for d, out_ref in enumerate(out_refs):
        first = ((my_x + d) & 3) * NZ

        def body(i, _):
            out_ref[i] = add_rows(a_ref, b_ref, first + i)
            return 0

        lax.fori_loop(0, NZ, body, 0, unroll=4)


def sum_body(a_ref, b_ref, c_ref, d_ref, out_ref):
    def body(i, _):
        low = a_ref[i].astype(f32) + b_ref[i].astype(f32)
        out_ref[i] = (low + (c_ref[i].astype(f32) + d_ref[i].astype(f32))).astype(bf16)
        return 0

    lax.fori_loop(0, NZ, body, 0, unroll=4)


def sum_lead_body(in_ref, out_ref):
    step = 16
    for t in range(out_ref.shape[0]):
        for r in range(0, out_ref.shape[1], step):
            rows = slice(r, r + step)
            total = in_ref[0, t, rows].astype(f32)
            for i in range(1, in_ref.shape[0]):
                total = total + in_ref[i, t, rows].astype(f32)
            out_ref[t, rows] = total.astype(bf16)


def spread(c, side):
    shape = (2 * c.shape[0], c.shape[0])
    r = lax.broadcasted_iota(jnp.int32, shape, 0)
    a = lax.broadcasted_iota(jnp.int32, shape, 1)
    pick = jnp.where((r >> 1) == a, 1.0, 0.0).astype(bf16)
    c = lax.dot_general(pick, c, (((1,), (side,)), ((), ())), preferred_element_type=f32)
    even = (r & 1) == 0
    return jnp.concatenate([jnp.where(even, c, 0.0), jnp.where(even, 0.0, c)], axis=1).astype(bf16)


def gather_rows(col_refs, t):
    return jnp.concatenate([r[t] for r in col_refs], axis=0)


def final_body(tens0_ref, tens1_ref, dens0_ref, dens1_ref, decay0_ref, decay1_ref, *refs):
    col_refs, grad_ref, mix_ref = refs[:-2], refs[-2], refs[-1]
    times = grad_ref.shape[0]

    @pl.when(pl.program_id(0) == 0)
    def _():
        for t in range(times):
            c = gather_rows(col_refs, t)
            for side in range(2):
                mix_ref[t, side] = spread(c, side)

    def scaled(refs, t):
        return jnp.concatenate(
            [(r[...].astype(f32) * f[pl.ds(t, 1), :]).astype(bf16) for r, f in zip(refs, (decay0_ref, decay1_ref))], axis=0
        )

    for t in range(times):
        g = jnp.dot(mix_ref[t, 0], scaled((tens0_ref, tens1_ref), t), preferred_element_type=f32)
        g = g + jnp.dot(mix_ref[t, 1], scaled((dens0_ref, dens1_ref), t), preferred_element_type=f32)
        grad_ref[t] = g.astype(bf16).reshape(g.shape[0] // 2, 2, g.shape[1])


def final(tens, dens, decay, collected):
    block, width = tens.shape
    times = decay.shape[0]
    half, step = width // 2, 512
    steps = half // step
    views = [pl.BlockSpec((block, step), lambda i, j=j: (0, i + j * steps)) for j in range(2)]
    decays = [pl.BlockSpec((times, step), lambda i, j=j: (0, i + j * steps)) for j in range(2)]
    whole = [pl.BlockSpec(c.shape, lambda i: (0, 0, 0)) for c in collected]
    return pl.pallas_call(
        final_body,
        grid=(steps,),
        out_shape=sds((times, block, 2, half)),
        in_specs=views * 2 + decays + whole,
        out_specs=pl.BlockSpec((times, block, 2, step), lambda i: (0, 0, 0, i)),
        scratch_shapes=[VMEM((times, 2, 2 * block, 2 * block), bf16)],
        cost_estimate=pl.CostEstimate(flops=10**9, bytes_accessed=4 << 20, transcendentals=0),
        compiler_params=pltpu.CompilerParams(vmem_limit_bytes=16 << 20),
        name="final",
    )(tens, tens, dens, dens, decay, decay, *collected)


def density_body(gram_ref, *refs):
    col_refs, out_ref = refs[:-1], refs[-1]
    tn = (((0,), (0,)), ((), ()))
    total = jnp.zeros((128, 256), f32)
    for t in range(2):
        c = gather_rows(col_refs, t)
        total = total + jnp.dot(c, gram_ref[t, 0], preferred_element_type=f32)
        total = total + lax.dot_general(c, gram_ref[t, 1], tn, preferred_element_type=f32)
    out_ref[...] = (total[:, 0:128] + total[:, 128:256]).astype(bf16)


def density_sum_body(a_ref, b_ref, c_ref, d_ref, out_ref):
    out_ref[...] = (a_ref[...].astype(f32) + b_ref[...].astype(f32)) + (c_ref[...].astype(f32) + d_ref[...].astype(f32))


def sds(shape, dtype=bf16):
    return jax.ShapeDtypeStruct(shape, dtype)


def exchange(value, groups):
    return lax.all_to_all(value, "blk", 0, 0, axis_index_groups=groups, tiled=True)


def work(chi_bar, cos_table, partner, tensor, dens_tensor, decay):
    pairs = chi_bar.shape[2]
    half = pairs // 2
    times = decay.shape[0]
    block = tensor.shape[0]
    width = tensor.shape[1] * tensor.shape[2]
    up, down = y_shift(1), y_shift(-1)

    chis = []
    start = 0
    for rows in CHUNKS:
        mine = [chi_bar[0, 0, h : h + half, start : start + rows, :] for h in (0, half)]
        low_a = lax.ppermute(mine[0], "tm", up)
        high_b = lax.ppermute(mine[1], "tm", down)
        low_b = lax.ppermute(mine[1], "tm", up)
        high_a = lax.ppermute(mine[0], "tm", down)
        far_a = lax.ppermute(low_a, "tm", up)
        far_b = lax.ppermute(high_b, "tm", down)
        chis.append((mine[0], low_a, high_a, far_a, mine[1], low_b, high_b, far_b))
        start += rows

    inputs = (tensor.reshape(block, width), dens_tensor.reshape(block, width), decay.reshape(times, width))
    metric, gram = call(
        prep_body, [sds((times, block, block)), sds((times, 2, block, 2 * block))], *inputs, flops=10**9
    )
    collected = []
    for c, rows in enumerate(CHUNKS):
        shape = sds((NX * NZ + 1, times, rows, block))
        piece = sds((NZ, times, rows, block))
        small = sds((times, rows, block))
        send, keep = call(term_body, [shape, shape], partner, cos_table, metric, *chis[c], smem=(0, 1), flops=10**9)
        other = lax.ppermute(send, "blk", CORE_SWAP)
        both = call(add_split_body, [piece] * NX, keep, other, flops=10**7)
        moved = [lax.ppermute(both[d], "blk", x_shift(d)) for d in range(1, NX)]
        both = call(sum_body, piece, both[0], *moved, flops=10**7)
        both = exchange(both, Z_GROUPS)
        collected.append(call(sum_lead_body, small, both, flops=10**7))
    dpart = call(density_body, sds((block, block)), gram, *collected, flops=10**8)
    parts = [lax.ppermute(dpart, "tm", y_shift(d)) for d in range(1, NY)]
    grad = final(*inputs, collected)
    density = call(density_sum_body, sds((block, block), f32), dpart, *parts)
    return (grad, density)


def solution(mesh):
    return jax.shard_map(
        work,
        mesh=mesh,
        in_specs=(
            P("tm", "blk", None, None, None),
            P(),
            P("blk", None),
            P("blk", None, None),
            P("blk", None, None),
            P("tm", None, None),
        ),
        out_specs=(P("tm", "blk", None, None), P("blk", None)),
        check_vma=False,
    )
```

```python
import math

import jax
import jax.numpy as jnp
from jax import lax
from jax.experimental import pallas as pl
from jax.experimental.pallas import tpu as pltpu
from jax.sharding import PartitionSpec as P


CHUNKS = (64, 64)
NX, NZ, NC, NY = 4, 8, 2, 4

bf16 = jnp.bfloat16
f32 = jnp.float32
VMEM = pltpu.VMEM
SMEM = pltpu.SMEM


def blk_of(x, z, c):
    return (x * NZ + z) * NC + c


CHIPS = [(x, z) for x in range(NX) for z in range(NZ)]
CORE_SWAP = [(blk_of(x, z, c), blk_of(x, z, 1 - c)) for x, z in CHIPS for c in range(NC)]
Z_GROUPS = [[blk_of(x, z, c) for z in range(NZ)] for x in range(NX) for c in range(NC)]


def x_shift(d):
    return [(blk_of(x, z, c), blk_of((x + d) % NX, z, c)) for x, z in CHIPS for c in range(NC)]


def y_shift(d):
    return [(i, (i + d) % NY) for i in range(NY)]


def call(body, out_shape, *args, smem=(), flops=0, mib=16):
    many = isinstance(out_shape, (list, tuple))
    size = sum(math.prod(a.shape) * a.dtype.itemsize for a in args)
    out_spec = pl.BlockSpec(memory_space=VMEM)
    return pl.pallas_call(
        body,
        out_shape=out_shape,
        in_specs=[pl.BlockSpec(memory_space=SMEM if i in smem else VMEM) for i in range(len(args))],
        out_specs=[out_spec] * len(out_shape) if many else out_spec,
        cost_estimate=pl.CostEstimate(flops=flops, bytes_accessed=size, transcendentals=0),
        compiler_params=pltpu.CompilerParams(vmem_limit_bytes=mib << 20),
    )(*args)


def prep_body(tens_ref, dens_ref, decay_ref, metric_ref, gram_ref):
    nt = (((1,), (1,)), ((), ()))
    inv_width = 1.0 / math.sqrt(tens_ref.shape[1])
    tens = tens_ref[...]
    for t in range(decay_ref.shape[0]):
        factor = decay_ref[pl.ds(t, 1), :]
        s = (tens.astype(f32) * factor).astype(bf16)
        d = (dens_ref[...].astype(f32) * factor).astype(bf16)
        m = lax.dot_general(tens, d, nt, preferred_element_type=f32)
        metric_ref[t] = (m * inv_width).astype(bf16)
        for i, left in enumerate((s, d)):
            g = lax.dot_general(left, d, nt, preferred_element_type=f32) * inv_width
            hi = g.astype(bf16)
            gram_ref[t, i, :, 0:128] = hi
            gram_ref[t, i, :, 128:256] = (g - hi.astype(f32)).astype(bf16)


def term_body(part_ref, cos_ref, metric_ref, *refs):
    chi_refs, (send_ref, keep_ref) = (refs[0:4], refs[4:8]), refs[8:]
    half, rows = refs[0].shape[0], refs[0].shape[1]
    group = 6
    me_y = lax.axis_index("tm")
    my_core = lax.axis_index("blk") & 1
    spare = keep_ref.shape[0] - 1
    zero = jnp.zeros((rows, 128), bf16)
    weights = [
        [cos_ref[me_y * 2 + t, (me_y + d) & 3].astype(f32) * (1.0 / 1024.0) for d in (0, 3, 1, 2)]
        for t in range(2)
    ]

    def clear(s, _):
        for t in range(2):
            send_ref[s, t] = zero
            keep_ref[s, t] = zero
        return 0

    lax.fori_loop(0, send_ref.shape[0], clear, 0)
    for k0 in range(0, 2 * half, group):
        ks = slice(k0 % half, k0 % half + group)
        chis = [r[ks].astype(f32) for r in chi_refs[k0 // half]]
        for t in range(2):
            mixed = chis[0] * weights[t][0]
            for i in range(1, 4):
                mixed = mixed + chis[i] * weights[t][i]
            mixed = mixed.astype(bf16).reshape(group * rows, 128)
            prod = jnp.dot(mixed, metric_ref[t], preferred_element_type=f32).astype(bf16)
            for j in range(group):
                p = part_ref[0, k0 + j]
                piece = prod[j * rows : (j + 1) * rows]
                own = (p & 1) == my_core
                keep_ref[jnp.where(own, p >> 1, spare), t] = piece
                send_ref[jnp.where(own, spare, p >> 1), t] = piece


def add_rows(a_ref, b_ref, i):
    return (a_ref[i].astype(f32) + b_ref[i].astype(f32)).astype(bf16)


def add_split_body(a_ref, b_ref, *out_refs):
    my_x = lax.axis_index("blk") >> 4
    for d, out_ref in enumerate(out_refs):
        first = ((my_x + d) & 3) * NZ

        def body(i, _):
            out_ref[i] = add_rows(a_ref, b_ref, first + i)
            return 0

        lax.fori_loop(0, NZ, body, 0, unroll=4)


def sum_body(a_ref, b_ref, c_ref, d_ref, out_ref):
    def body(i, _):
        low = a_ref[i].astype(f32) + b_ref[i].astype(f32)
        out_ref[i] = (low + (c_ref[i].astype(f32) + d_ref[i].astype(f32))).astype(bf16)
        return 0

    lax.fori_loop(0, NZ, body, 0, unroll=4)


def sum_lead_body(in_ref, out_ref):
    step = 16
    for t in range(out_ref.shape[0]):
        for r in range(0, out_ref.shape[1], step):
            rows = slice(r, r + step)
            total = in_ref[0, t, rows].astype(f32)
            for i in range(1, in_ref.shape[0]):
                total = total + in_ref[i, t, rows].astype(f32)
            out_ref[t, rows] = total.astype(bf16)


def spread(c, side):
    shape = (2 * c.shape[0], c.shape[0])
    r = lax.broadcasted_iota(jnp.int32, shape, 0)
    a = lax.broadcasted_iota(jnp.int32, shape, 1)
    pick = jnp.where((r >> 1) == a, 1.0, 0.0).astype(bf16)
    c = lax.dot_general(pick, c, (((1,), (side,)), ((), ())), preferred_element_type=f32)
    even = (r & 1) == 0
    return jnp.concatenate([jnp.where(even, c, 0.0), jnp.where(even, 0.0, c)], axis=1).astype(bf16)


def gather_rows(col_refs, t):
    return jnp.concatenate([r[t] for r in col_refs], axis=0)


def final_body(tens0_ref, tens1_ref, dens0_ref, dens1_ref, decay0_ref, decay1_ref, *refs):
    col_refs, grad_ref, mix_ref = refs[:-2], refs[-2], refs[-1]
    times = grad_ref.shape[0]

    @pl.when(pl.program_id(0) == 0)
    def _():
        for t in range(times):
            c = gather_rows(col_refs, t)
            for side in range(2):
                mix_ref[t, side] = spread(c, side)

    def scaled(refs, t):
        return jnp.concatenate(
            [(r[...].astype(f32) * f[pl.ds(t, 1), :]).astype(bf16) for r, f in zip(refs, (decay0_ref, decay1_ref))], axis=0
        )

    for t in range(times):
        g = jnp.dot(mix_ref[t, 0], scaled((tens0_ref, tens1_ref), t), preferred_element_type=f32)
        g = g + jnp.dot(mix_ref[t, 1], scaled((dens0_ref, dens1_ref), t), preferred_element_type=f32)
        grad_ref[t] = g.astype(bf16).reshape(g.shape[0] // 2, 2, g.shape[1])


def final(tens, dens, decay, collected):
    block, width = tens.shape
    times = decay.shape[0]
    half, step = width // 2, 1024
    steps = half // step
    views = [pl.BlockSpec((block, step), lambda i, j=j: (0, i + j * steps)) for j in range(2)]
    decays = [pl.BlockSpec((times, step), lambda i, j=j: (0, i + j * steps)) for j in range(2)]
    whole = [pl.BlockSpec(c.shape, lambda i: (0, 0, 0)) for c in collected]
    return pl.pallas_call(
        final_body,
        grid=(steps,),
        out_shape=sds((times, block, 2, half)),
        in_specs=views * 2 + decays + whole,
        out_specs=pl.BlockSpec((times, block, 2, step), lambda i: (0, 0, 0, i)),
        scratch_shapes=[VMEM((times, 2, 2 * block, 2 * block), bf16)],
        cost_estimate=pl.CostEstimate(flops=10**9, bytes_accessed=4 << 20, transcendentals=0),
        compiler_params=pltpu.CompilerParams(vmem_limit_bytes=16 << 20),
        name="final",
    )(tens, tens, dens, dens, decay, decay, *collected)


def density_body(gram_ref, *refs):
    col_refs, out_ref = refs[:-1], refs[-1]
    tn = (((0,), (0,)), ((), ()))
    total = jnp.zeros((128, 256), f32)
    for t in range(2):
        c = gather_rows(col_refs, t)
        total = total + jnp.dot(c, gram_ref[t, 0], preferred_element_type=f32)
        total = total + lax.dot_general(c, gram_ref[t, 1], tn, preferred_element_type=f32)
    out_ref[...] = (total[:, 0:128] + total[:, 128:256]).astype(bf16)


def density_sum_body(a_ref, b_ref, c_ref, d_ref, out_ref):
    out_ref[...] = (a_ref[...].astype(f32) + b_ref[...].astype(f32)) + (c_ref[...].astype(f32) + d_ref[...].astype(f32))


def sds(shape, dtype=bf16):
    return jax.ShapeDtypeStruct(shape, dtype)


def exchange(value, groups):
    return lax.all_to_all(value, "blk", 0, 0, axis_index_groups=groups, tiled=True)


def work(chi_bar, cos_table, partner, tensor, dens_tensor, decay):
    pairs = chi_bar.shape[2]
    half = pairs // 2
    times = decay.shape[0]
    block = tensor.shape[0]
    width = tensor.shape[1] * tensor.shape[2]
    up, down = y_shift(1), y_shift(-1)

    chis = []
    start = 0
    for c, rows in enumerate(CHUNKS):
        if c:
            chi_bar = lax.optimization_barrier((chi_bar, mine))[0]
        mine = [chi_bar[0, 0, h : h + half, start : start + rows, :] for h in (0, half)]
        low_a = lax.ppermute(mine[0], "tm", up)
        high_b = lax.ppermute(mine[1], "tm", down)
        low_b = lax.ppermute(mine[1], "tm", up)
        high_a = lax.ppermute(mine[0], "tm", down)
        far_a = lax.ppermute(low_a, "tm", up)
        far_b = lax.ppermute(high_b, "tm", down)
        chis.append((mine[0], low_a, high_a, far_a, mine[1], low_b, high_b, far_b))
        start += rows

    inputs = (tensor.reshape(block, width), dens_tensor.reshape(block, width), decay.reshape(times, width))
    metric, gram = call(
        prep_body, [sds((times, block, block)), sds((times, 2, block, 2 * block))], *inputs, flops=10**9
    )
    collected = []
    for c, rows in enumerate(CHUNKS):
        shape = sds((NX * NZ + 1, times, rows, block))
        piece = sds((NZ, times, rows, block))
        small = sds((times, rows, block))
        send, keep = call(term_body, [shape, shape], partner, cos_table, metric, *chis[c], smem=(0, 1), flops=10**9)
        other = lax.ppermute(send, "blk", CORE_SWAP)
        both = call(add_split_body, [piece] * NX, keep, other, flops=10**7)
        moved = [lax.ppermute(both[d], "blk", x_shift(d)) for d in range(1, NX)]
        both = call(sum_body, piece, both[0], *moved, flops=10**7)
        both = exchange(both, Z_GROUPS)
        collected.append(call(sum_lead_body, small, both, flops=10**7))
    dpart = call(density_body, sds((block, block)), gram, *collected, flops=10**8)
    parts = [lax.ppermute(dpart, "tm", y_shift(d)) for d in range(1, NY)]
    grad = final(*inputs, collected)
    density = call(density_sum_body, sds((block, block), f32), dpart, *parts)
    return (grad, density)


def solution(mesh):
    return jax.shard_map(
        work,
        mesh=mesh,
        in_specs=(
            P("tm", "blk", None, None, None),
            P(),
            P("blk", None),
            P("blk", None, None),
            P("blk", None, None),
            P("tm", None, None),
        ),
        out_specs=(P("tm", "blk", None, None), P("blk", None)),
        check_vma=False,
    )
```
